32 devices in a mesh: fsdp: 4 (over y, x), ep: 8 (over z, core).
Axes of the slice: x: 2, y: 2, z: 4, core: 2. Of those that a mesh axis runs over, the one named last changes fastest.
Arguments:
- hidden_in: bfloat16 [8192, 2048], P(('fsdp', 'ep')), may hold values from -6 to 6
- norm_gain: float32 [2048], replicated, may hold values from 0.25 to 1.75
- expert_ids: int32 [8192, 8], P(('fsdp', 'ep')), may hold values from 0 to 15, all different within a row; in each aligned block of 256 rows (0 to 255, 256 to 511, ...) at most 160 rows name the same one
- expert_probs: float32 [8192, 8], P(('fsdp', 'ep')), may hold values from 0.05 to 0.25
- gate_proj: bfloat16 [16, 2048, 768], P('ep', 'fsdp'), may hold values from -0.125 to 0.125
- up_proj: bfloat16 [16, 2048, 768], P('ep', 'fsdp'), may hold values from -0.125 to 0.125
- down_proj: bfloat16 [16, 768, 2048], P('ep', None, 'fsdp'), may hold values from -0.21875 to 0.21875
Outputs:
- moe_out: bfloat16 [8192, 2048], P(('fsdp', 'ep'))
The draws below stay inside these ranges and needn't reach their ends.
Inputs may be any that keep to these rules, and one draw needn't show every extreme that they name: `expert_ids`: within the rows of one device (aligned blocks of 256 rows) each expert id is named by at most 160 rows, and in some blocks one expert by exactly 160; the 8 ids of a row are distinct.
All inputs are finite; a program needn't handle non-finite values.
Results may differ from the reference program's by a relative error of at most 0.0025.
Values may be sent and summed in bfloat16 or wider, within the bound.
A program may use at most 128 MiB of HBM per device.

```python
import math
import jax
import jax.numpy as jnp
import numpy as np
from jax import lax

D = 2048
FF = 768
TOP = 8
TOK_DEV = 256
EXPERTS = 16
CAP = 160
TOKENS = 8192


def levels(key, dims, pieces, low, high):
    level = 1.0
    for dim, blocks in pieces:
        draws = jax.random.uniform(jax.random.fold_in(jax.random.fold_in(key, 6), dim), (blocks,), jnp.float32, low / len(pieces), high / len(pieces))
        level = level * jnp.repeat(jnp.exp(draws), dims[dim] // blocks).reshape((-1,) + (1,) * (len(dims) - 1 - dim))
    return level


def assign_block(rng, own, number, rows, amount, top, reach, lean):
    sequence = jax.random.permutation(rng, amount)
    packed, ordinary = load_shares(amount, rows * top, reach, lean, True), load_shares(amount, rows * top, reach, lean, False)
    places = jnp.arange(amount)

    def named(sizes, turn):
        used = int((sizes > 0).sum())
        fixed = max(1, used // 4)
        shifted = fixed + (places - fixed + turn * (used - fixed)) % max(1, amount - fixed)
        return jnp.zeros((amount,), jnp.int32).at[sequence[jnp.where(places < fixed, places, shifted)]].set(jnp.asarray(sizes, jnp.int32))

    sizes = jnp.where(number % 4 == 0, named(packed, number // 4), named(ordinary, number - number // 4 - 1))
    mixed = jax.random.permutation(jax.random.fold_in(own, 3), amount)
    source_of, taker = mixed[0:amount // 2 * 2:2], mixed[1:amount // 2 * 2:2]
    slack = jnp.minimum(sizes[source_of] - 1, reach - sizes[taker]) // 2
    slack = jnp.where((source_of == sequence[0]) | (taker == sequence[0]) | (sizes[taker] == 0), 0, jnp.maximum(slack, 0))
    shifted = jax.random.randint(jax.random.fold_in(own, 4), (amount // 2,), 0, 1 << 20) % (slack + 1)
    sizes = sizes.at[source_of].add(-shifted).at[taker].add(shifted)
    members = jnp.searchsorted(jnp.cumsum(sizes), jnp.arange(rows * top), side="right").astype(jnp.int32)
    table = members.reshape(top, rows).T
    table = table[jax.random.permutation(jax.random.fold_in(own, 1), rows)]
    turn = jax.random.randint(jax.random.fold_in(own, 2), (rows, 1), 0, top)
    return jnp.take_along_axis(table, (jnp.arange(top)[None, :] + turn) % top, axis=1)


def load_shares(number_of, total, limit, slope, full):
    weights = [(1 << 20) // math.isqrt(standing ** slope) + 1 for standing in range(1, number_of + 1)]
    largest = limit if full else min(limit, max(-(-total // number_of), total * weights[0] // sum(weights)))
    least = 1 if total - largest >= number_of - 1 else 0
    holding, spare = [largest] + [least] * (number_of - 1), total - largest - least * (number_of - 1)
    while spare > 0:
        movable = [i for i in range(1, number_of) if holding[i] < largest] or [i for i in range(1, number_of) if holding[i] < limit]
        pool, remaining = sum([weights[i] for i in movable]), spare
        for i in movable:
            addition = min(limit - holding[i], max(1, remaining * weights[i] // pool), spare)
            holding[i] = holding[i] + addition
            spare = spare - addition
    return np.array(holding)


def normal_values(key, extent, deviation, bound, split=(), held_as=jnp.bfloat16):
    gain = levels(key, extent, split, -0.22, 0.18) if split else 1.0
    result = jax.random.normal(key, extent, jnp.float32) * deviation * gain
    return jnp.minimum(jnp.maximum(result, -bound), bound).astype(held_as)


def setup_inputs(seed: int = 0) -> dict:
    key_list = jax.random.split(jax.random.key(seed), 8)
    hidden_in = normal_values(key_list[0], (TOKENS, D), 1.0, 6.0, ((0, 32),))
    norm_gain = jnp.clip(1.0 + 0.15 * jax.random.normal(key_list[1], (D,), jnp.float32), 0.25, 1.75)
    expert_ids_keys = jax.random.split(jax.random.fold_in(key_list[2], 1), TOKENS // TOK_DEV)
    expert_ids_turns = jax.random.permutation(jax.random.fold_in(key_list[2], 3), TOKENS // TOK_DEV)
    expert_ids = jax.vmap(lambda own, number: assign_block(jax.random.fold_in(key_list[2], 2), own, number, TOK_DEV, EXPERTS, TOP, CAP, 1))(expert_ids_keys, expert_ids_turns).reshape((TOKENS, TOP))
    expert_probs = jnp.clip(0.05 + 0.2 * jax.random.uniform(key_list[3], (TOKENS, TOP), jnp.float32) ** levels(key_list[3], (TOKENS, TOP), ((0, 32),), -0.2, 0.2), 0.05, 0.25)
    gate_proj = normal_values(key_list[4], (EXPERTS, D, FF), D ** -0.5, 0.125, ((0, 8), (1, 4)))
    up_proj = normal_values(key_list[5], (EXPERTS, D, FF), D ** -0.5, 0.125, ((0, 8), (1, 4)))
    down_proj = normal_values(key_list[6], (EXPERTS, FF, D), FF ** -0.5, 0.21875, ((0, 8), (2, 4)))
    return {"hidden_in": hidden_in, "norm_gain": norm_gain, "expert_ids": expert_ids, "expert_probs": expert_probs, "gate_proj": gate_proj, "up_proj": up_proj, "down_proj": down_proj}


def rms_norm(hidden_in, norm_gain):
    values = hidden_in.astype(jnp.float32)
    spread = lax.optimization_barrier(jnp.mean(values * values, axis=-1, keepdims=True))
    return (values * lax.rsqrt(spread + 1e-06) * norm_gain).astype(jnp.bfloat16)

def block_slots(ids_row):
    onehot = (ids_row[:, None] == jnp.arange(EXPERTS, dtype=jnp.int32)[None, :]).astype(jnp.int32)
    before = jnp.cumsum(onehot, axis=0) - onehot
    return (ids_row * CAP + lax.optimization_barrier(jnp.sum(before * onehot, axis=1))).astype(jnp.int32)

def reference(hidden_in, norm_gain, expert_ids, expert_probs, gate_proj, up_proj, down_proj):
    normed = rms_norm(hidden_in, norm_gain)
    blocks = TOKENS // TOK_DEV
    block_ids = expert_ids.reshape(blocks, TOK_DEV * TOP).astype(jnp.int32)
    slot_index = jax.vmap(block_slots)(block_ids)
    block_base = (jnp.arange(blocks, dtype=jnp.int32) * TOK_DEV)[:, None]
    token_of = block_base + (jnp.arange(TOK_DEV * TOP, dtype=jnp.int32) // TOP)[None, :]
    row_index = jnp.arange(blocks, dtype=jnp.int32)[:, None]
    source = jnp.zeros((blocks, EXPERTS * CAP), jnp.int32).at[row_index, slot_index].set(token_of)
    weights = jnp.zeros((blocks, EXPERTS * CAP), jnp.float32).at[row_index, slot_index].set(expert_probs.reshape(blocks, TOK_DEV * TOP).astype(jnp.float32))
    source = source.reshape(blocks, EXPERTS, CAP).transpose(1, 0, 2).reshape(EXPERTS, blocks * CAP)
    weights = weights.reshape(blocks, EXPERTS, CAP).transpose(1, 0, 2).reshape(EXPERTS, blocks * CAP)

    def one_expert(running, inputs):
        src_rows, slot_weights, w_gate, w_upper, w_lower = inputs
        gathered = normed[src_rows]
        gate = jnp.dot(gathered, w_gate, preferred_element_type=jnp.float32)
        upper = jnp.dot(gathered, w_upper, preferred_element_type=jnp.float32)
        activated = (jax.nn.silu(gate) * upper).astype(jnp.bfloat16)
        output = jnp.dot(activated, w_lower, preferred_element_type=jnp.float32).astype(jnp.bfloat16)
        running = running.at[src_rows].add(slot_weights[:, None] * output.astype(jnp.float32))
        return (running, None)
    running = jnp.zeros((TOKENS, D), jnp.float32)
    running, unused = lax.scan(one_expert, running, (source, weights, gate_proj, up_proj, down_proj))
    return running.astype(jnp.bfloat16)
```

```python
import jax
import jax.numpy as jnp
from jax import lax
from jax.sharding import PartitionSpec as P


def rms_norm(hidden_in, norm_gain):
    values = hidden_in.astype(jnp.float32)
    spread = jnp.mean(values * values, axis=-1, keepdims=True)
    return (values * lax.rsqrt(spread + 1e-06) * norm_gain).astype(jnp.bfloat16)


def per_device(hidden_in, norm_gain, expert_ids, expert_probs, gate_proj, up_proj, down_proj):
    local_experts = gate_proj.shape[0]
    normed = rms_norm(hidden_in, norm_gain)
    all_experts = local_experts * lax.axis_size("ep")
    hot = expert_ids[:, :, None] == jnp.arange(all_experts, dtype=jnp.int32)
    weights = jnp.sum(jnp.where(hot, expert_probs[:, :, None], 0.0), axis=1)
    tokens = lax.all_gather(normed, "ep", axis=0, tiled=True)
    routed = lax.all_to_all(
        weights.reshape(weights.shape[0], lax.axis_size("ep"), local_experts),
        "ep", split_axis=1, concat_axis=0, tiled=True,
    ).reshape(tokens.shape[0], local_experts)
    total = 0.0
    gate_all = lax.all_gather(gate_proj, "fsdp", axis=1, tiled=True)
    up_all = lax.all_gather(up_proj, "fsdp", axis=1, tiled=True)
    down_all = lax.all_gather(down_proj, "fsdp", axis=2, tiled=True)
    for e in range(local_experts):
        gate = jnp.dot(tokens, gate_all[e], preferred_element_type=jnp.float32)
        up = jnp.dot(tokens, up_all[e], preferred_element_type=jnp.float32)
        act = (jax.nn.silu(gate) * up).astype(jnp.bfloat16)
        out = jnp.dot(act, down_all[e], preferred_element_type=jnp.float32).astype(jnp.bfloat16)
        total = total + out.astype(jnp.float32) * routed[:, e, None]
    combined = lax.psum_scatter(total, "ep", scatter_dimension=0, tiled=True)
    return combined.astype(jnp.bfloat16)


def solution(mesh):
    return jax.shard_map(
        per_device,
        mesh=mesh,
        in_specs=(
            P(("fsdp", "ep"), None),
            P(),
            P(("fsdp", "ep"), None),
            P(("fsdp", "ep"), None),
            P("ep", "fsdp", None),
            P("ep", "fsdp", None),
            P("ep", None, "fsdp"),
        ),
        out_specs=P(("fsdp", "ep"), None),
        check_vma=False,
    )
```

```python
import functools

import jax
import jax.numpy as jnp
from jax import lax
from jax.experimental import pallas as pl
from jax.experimental.pallas import tpu as pltpu
from jax.sharding import PartitionSpec as P


WEIGHT_LIMIT, PROB_LIMIT = 0.21875, 0.25


def rms_norm(hidden_in, norm_gain):
    values = hidden_in.astype(jnp.float32)
    spread = jnp.mean(values * values, axis=-1, keepdims=True)
    return (values * lax.rsqrt(spread + 1e-06) * norm_gain).astype(jnp.bfloat16)


def flip(value, size, bit):
    return lax.ppermute(value, "fsdp", [(i, i ^ bit) for i in range(size)])


def gather_pair(left, right, size):
    if size != 4:
        whole = [lax.all_gather(part, "fsdp", axis=0) for part in (left, right)]
        return [[part[i] for i in range(size)] for part in whole]

    def move(value, bit):
        return flip(value, size, bit)

    left_one, right_two = move(left, 1), move(right, 2)
    left_two, right_one = move(left, 2), move(right, 1)
    left_far, right_far = move(left_two, 1), move(right_one, 2)
    return [left, left_one, left_two, left_far], [right, right_one, right_two, right_far]


def hidden_kernel(count, place, x_ref, *refs):
    gates, ups = refs[:count], refs[count:2 * count]
    act_ref, peak_ref, gate_all, up_all = refs[2 * count:]
    depth = gates[0].shape[0]

    @pl.when(pl.program_id(0) == 0)
    def _():
        for k in range(count):
            rows = pl.ds(pl.multiple_of(place[k] * depth, depth), depth)
            gate_all[rows, :] = gates[k][...]
            up_all[rows, :] = ups[k][...]

    gate = jnp.dot(x_ref[...], gate_all[...], preferred_element_type=jnp.float32)
    up = jnp.dot(x_ref[...], up_all[...], preferred_element_type=jnp.float32)
    act = gate / (1.0 + jnp.exp(-gate)) * up
    act_ref[...] = act.astype(jnp.bfloat16)
    peak = jnp.max(jnp.abs(act), axis=0, keepdims=True)
    peak_ref[...] = jnp.broadcast_to(jnp.max(peak, axis=1, keepdims=True), peak_ref.shape[1:])[None]


def hidden(tokens, gates, ups, place):
    count = len(gates)
    rows, width = tokens.shape
    depth, units = gates[0].shape
    tile = min(512, rows)
    weight_spec = pl.BlockSpec((depth, units), lambda t, place: (0, 0))
    return pl.pallas_call(
        functools.partial(hidden_kernel, count),
        grid_spec=pltpu.PrefetchScalarGridSpec(
            num_scalar_prefetch=1,
            grid=(rows // tile,),
            in_specs=[pl.BlockSpec((tile, width), lambda t, place: (t, 0))]
            + [weight_spec] * (2 * count),
            out_specs=[
                pl.BlockSpec((tile, units), lambda t, place: (t, 0)),
                pl.BlockSpec((1, 8, 128), lambda t, place: (t, 0, 0)),
            ],
            scratch_shapes=[pltpu.VMEM((width, units), jnp.bfloat16)] * 2,
        ),
        out_shape=[
            jax.ShapeDtypeStruct((rows, units), jnp.bfloat16),
            jax.ShapeDtypeStruct((rows // tile, 8, 128), jnp.float32),
        ],
        cost_estimate=pl.CostEstimate(
            flops=4 * rows * width * units,
            bytes_accessed=2 * rows * (width + units),
            transcendentals=rows * units,
        ),
        name="hidden",
    )(place, tokens, *gates, *ups)


def down_kernel(count, *refs):
    acts, shares = refs[:2 * count], refs[2 * count:2 * count + 2]
    weights, outs = refs[2 * count + 2:3 * count + 2], refs[3 * count + 2:]
    for side in range(2):
        total = None
        for e in range(count):
            one = jnp.dot(acts[2 * e + side][...], weights[e][...], preferred_element_type=jnp.float32)
            one = one.astype(jnp.bfloat16).astype(jnp.float32) * shares[side][:, e:e + 1]
            total = one if total is None else total + one
        outs[side][0] = total


def down(acts, routed, pieces, block):
    count = len(acts)
    rows, units = acts[0].shape
    width = pieces[0].shape[1]
    chips = rows // block // 2
    out = jax.ShapeDtypeStruct((chips, block, width), jnp.float32)
    sides = [lambda k: (2 * k, 0), lambda k: (2 * k + 1, 0)]
    return pl.pallas_call(
        functools.partial(down_kernel, count),
        grid=(chips,),
        in_specs=[pl.BlockSpec((block, units), side) for _ in range(count) for side in sides]
        + [pl.BlockSpec((block, count), side) for side in sides]
        + [pl.BlockSpec((units, width), lambda k: (0, 0))] * count,
        out_specs=[pl.BlockSpec((1, block, width), lambda k: (k, 0, 0))] * 2,
        out_shape=[out, out],
        cost_estimate=pl.CostEstimate(
            flops=2 * count * rows * width * units,
            bytes_accessed=2 * count * rows * units + 4 * rows * width,
            transcendentals=0,
        ),
        name="down",
    )(*[act for act in acts for _ in range(2)], routed, routed, *pieces)


def layer(hidden_in, norm_gain, expert_ids, expert_probs, gate_proj, up_proj, down_proj):
    local_experts = gate_proj.shape[0]
    block, width = hidden_in.shape
    groups, shards = lax.axis_size("ep"), lax.axis_size("fsdp")
    chips = groups // 2
    me = lax.axis_index("ep")
    z, core = me // 2, me % 2
    own = lax.axis_index("fsdp")
    sibling = [(i, i ^ 1) for i in range(groups)]

    normed = rms_norm(hidden_in, norm_gain)
    hot = expert_ids[:, :, None] == jnp.arange(local_experts * groups, dtype=jnp.int32)
    weights = jnp.sum(jnp.where(hot, expert_probs[:, :, None], 0.0), axis=1)

    routed_all = lax.all_gather(weights, "ep", axis=0)
    normed, routed_all = lax.optimization_barrier((normed, routed_all))

    def hop(value, step, way):
        first = range(step - 1, chips - 1) if way > 0 else range(1, chips - step + 1)
        pairs = [(2 * i + c, 2 * (i + way) + c) for i in first for c in range(2)]
        return lax.ppermute(value, "ep", pairs)

    up_way, down_way = [normed], [normed]
    for step in range(1, chips):
        up_way.append(hop(up_way[-1], step, 1))
        down_way.append(hop(down_way[-1], step, -1))
    same = [normed] + [
        jnp.where(z >= k, up_way[k], down_way[chips - k]) for k in range(1, chips)
    ]
    other = [lax.ppermute(part, "ep", sibling) for part in same]
    tokens = jnp.concatenate([part for k in range(chips) for part in (same[k], other[k])], axis=0)
    routed_own = lax.dynamic_slice_in_dim(routed_all, me * local_experts, local_experts, 2)
    chip_of = jnp.mod(z - jnp.arange(chips), chips)
    order = jnp.stack([2 * chip_of + core, 2 * chip_of + 1 - core], axis=1).reshape(-1)
    routed = routed_own[order].reshape(groups * block, local_experts)

    if shards == 4:
        place = own ^ jnp.arange(shards, dtype=jnp.int32)
    else:
        place = jnp.arange(shards, dtype=jnp.int32)
    pairs = [gather_pair(gate_proj[e], up_proj[e], shards) for e in range(local_experts)]
    halves = [
        gather_pair(down_proj[e], down_proj[e + 1], shards)
        for e in range(0, local_experts, 2)
    ]
    downs = [part for half in halves for part in half]
    acts, peaks = [], []
    for pair in pairs:
        act, peak = hidden(tokens, *pair, place)
        acts.append(act)
        peaks.append(jnp.max(peak, axis=0))
    level = functools.reduce(jnp.maximum, peaks)
    level = jnp.maximum(level, lax.ppermute(level, "ep", sibling))
    units = acts[0].shape[1]
    level = jnp.maximum(level, 1e-25) * (WEIGHT_LIMIT * PROB_LIMIT * units * 2 * local_experts / 2**15)
    levels = [level] + [
        lax.ppermute(level, "ep", [(i, (i - 2 * k) % groups) for i in range(groups)])
        for k in range(1, chips)
    ]
    shrink = 1.0 / level[0, 0]

    out = jnp.zeros((block, width), jnp.bfloat16)
    depth = down_proj.shape[2]
    sent = []
    for shard in range(shards):
        ready = acts
        if shard > 1:
            ready, sent[shard - 2] = lax.optimization_barrier((acts, sent[shard - 2]))
        mine, theirs = down(ready, routed, [part[shard] for part in downs], block)
        chip_sum = mine + lax.ppermute(theirs, "ep", sibling)
        sent.append((chip_sum[0], [(chip_sum[k] * shrink).astype(jnp.float16) for k in range(1, chips)]))
    for shard in range(shards):
        total, parts = sent[shard]
        for k in range(1, chips):
            back = [(i, (i - 2 * k) % groups) for i in range(groups)]
            part = lax.ppermute(parts[k - 1], "ep", back)
            total = total + part.astype(jnp.float32) * levels[k][0, 0]
        out = lax.dynamic_update_slice(out, total.astype(jnp.bfloat16), (0, place[shard] * depth))
    return out


def solution(mesh):
    return jax.shard_map(
        layer,
        mesh=mesh,
        in_specs=(
            P(("fsdp", "ep"), None),
            P(),
            P(("fsdp", "ep"), None),
            P(("fsdp", "ep"), None),
            P("ep", "fsdp", None),
            P("ep", "fsdp", None),
            P("ep", None, "fsdp"),
        ),
        out_specs=P(("fsdp", "ep"), None),
        check_vma=False,
    )
```
